32 devices in a mesh: row: 4 (over y, x), col: 8 (over z, core).
Axes of the slice: x: 2, y: 2, z: 4, core: 2. Of those that a mesh axis runs over, the one named last changes fastest.
Arguments:
- tokens: bfloat16 [4096, 3584], P(('row', 'col')), may hold values from -6 to 6
- targets: bfloat16 [4096, 3584], P(('row', 'col')), may hold values from -6 to 6
- w_up: bfloat16 [8, 3584, 448], P('col', 'row'), may hold values from -6 to 6
- w_down: bfloat16 [4, 3584, 448], P('row', 'col'), may hold values from -6 to 6
- up_momentum: float32 [8, 3584, 448], P('col', 'row'), may hold values from -2 to 2
- down_momentum: float32 [4, 3584, 448], P('row', 'col'), may hold values from -2 to 2
- member_up: int32 [4, 8], replicated, may hold values from 0 to 1, as said below
- member_down: int32 [4, 8], replicated, may hold values from 0 to 1, as said below
- path_rate: float32 [4, 8], replicated, may hold values from 0.1 to 1
Outputs:
- new_up: bfloat16 [8, 3584, 448], P('col', 'row')
- new_up_momentum: float32 [8, 3584, 448], P('col', 'row')
- new_down: bfloat16 [4, 3584, 448], P('row', 'col')
- new_down_momentum: float32 [4, 3584, 448], P('row', 'col')
The draws below stay inside these ranges and needn't reach their ends.
Inputs may be any that keep to these rules, and one draw needn't show every extreme that they name: Every column of member_up holds at least one 1. Every row of member_down holds at least one 1.
All inputs are finite; a program needn't handle non-finite values. Where the reference program divides by a largest or mean magnitude, that divisor is 1e-20 or more.
Results may differ from the reference program's by a relative error of at most 0.006.
Values may be sent and summed in bfloat16 or wider, within the bound.
No kernel may reach another device: no remote copies, remote signals or barrier semaphores. Data moves between devices by JAX's collectives and lax.ppermute only.
A program may use at most 64 MiB of HBM per device.

```python
import math
import jax
import jax.numpy as jnp
from jax import lax

D = 3584
H = 448
ROWS = 128
TOKENS = 4096
UP_MODULES = 8
DOWN_MODULES = 4
N_ROW = 4
N_COL = 8


def draw_member_up(key, part):
    first, second = jax.random.split(jax.random.fold_in(key, 11))
    flags = jax.random.randint(first, (N_ROW, N_COL), 0, 2).astype(jnp.int32)
    chosen = jax.random.randint(second, (1, N_COL), 0, N_ROW).astype(jnp.int32)
    places = lax.broadcasted_iota(jnp.int32, (N_ROW, N_COL), 0)
    return jnp.maximum(flags, (places == chosen).astype(jnp.int32))


def draw_member_down(key, part):
    first, second = jax.random.split(jax.random.fold_in(key, 23))
    flags = jax.random.randint(first, (N_ROW, N_COL), 0, 2).astype(jnp.int32)
    chosen = jax.random.randint(second, (N_ROW, 1), 0, N_COL).astype(jnp.int32)
    places = lax.broadcasted_iota(jnp.int32, (N_ROW, N_COL), 1)
    return jnp.maximum(flags, (places == chosen).astype(jnp.int32))


def shard_levels(own_key, dims, cuts, smallest, top_value):
    def one(dim, parts):
        draws = jax.random.uniform(jax.random.fold_in(jax.random.fold_in(own_key, 6), dim), (parts,), jnp.float32, smallest / len(cuts), top_value / len(cuts))
        return jnp.repeat(jnp.exp(draws), dims[dim] // parts).reshape((-1,) + (1,) * (len(dims) - dim - 1))

    level = one(*cuts[0])
    for cut in cuts[1:]:
        level = level * one(*cut)
    return level


def scatter_about(own_key, extent, deviation, reach, pieces=(), held_as=jnp.bfloat16):
    result = deviation * jax.random.normal(own_key, extent, jnp.float32)
    if pieces:
        result = result * shard_levels(own_key, extent, pieces, -0.22, 0.18)
    return jnp.clip(result, -reach, reach).astype(held_as)


def setup_inputs(seed: int = 0) -> dict:
    arg_keys = jax.random.split(jax.random.key(seed), 10)
    tokens = scatter_about(arg_keys[0], (TOKENS, D), 1.0, 6.0, ((0, 32),))
    targets = scatter_about(arg_keys[1], (TOKENS, D), 1.0, 6.0, ((0, 32),))
    w_up = scatter_about(arg_keys[2], (UP_MODULES, D, H), 1.0, 6.0, ((0, 8), (1, 4)))
    w_down = scatter_about(arg_keys[3], (DOWN_MODULES, D, H), 1.0, 6.0, ((0, 4), (1, 8)))
    up_momentum = scatter_about(arg_keys[4], (UP_MODULES, D, H), 0.3, 2.0, ((0, 8), (1, 4)), jnp.float32)
    down_momentum = scatter_about(arg_keys[5], (DOWN_MODULES, D, H), 0.3, 2.0, ((0, 4), (1, 8)), jnp.float32)
    member_up = draw_member_up(jax.random.fold_in(arg_keys[9], 71), 0)
    member_down = draw_member_down(jax.random.fold_in(arg_keys[9], 71), 0)
    path_rate = jnp.clip(jnp.exp(jax.random.uniform(arg_keys[8], (N_ROW, N_COL), jnp.float32, math.log(0.1), math.log(1.0))), 0.1, 1.0)
    return {"tokens": tokens, "targets": targets, "w_up": w_up, "w_down": w_down, "up_momentum": up_momentum, "down_momentum": down_momentum, "member_up": member_up, "member_down": member_down, "path_rate": path_rate}


def silu_slope(pre):
    sig = jax.nn.sigmoid(pre)
    return sig * (1.0 + pre * (1.0 - sig))

def forward(tokens_path, targets_path, up_matrix, down_matrix):
    pre = jnp.dot(tokens_path, up_matrix, preferred_element_type=jnp.float32) * D ** (-0.5)
    hidden_act = jax.nn.silu(pre).astype(jnp.bfloat16)
    mixed = lax.dot_general(hidden_act, down_matrix, (((1,), (1,)), ((), ())), preferred_element_type=jnp.float32) * H ** (-0.5)
    slope_out = (tokens_path.astype(jnp.float32) + mixed - targets_path.astype(jnp.float32)).astype(jnp.bfloat16)
    return (pre, hidden_act, slope_out)

def packed(grad, rate):
    spread = jnp.sqrt(lax.optimization_barrier(jnp.mean(grad * grad, axis=1, keepdims=True)) + 1e-05)
    unit = grad / (jnp.abs(grad) + spread)
    largest = lax.optimization_barrier(jnp.max(jnp.abs(unit), axis=1, keepdims=True)) + 1e-06
    return ((unit / largest).astype(jnp.bfloat16), rate * largest[:, 0])

def grad_up(tokens_path, targets_path, up_matrix, down_matrix):
    pre, hidden_act, slope_out = forward(tokens_path, targets_path, up_matrix, down_matrix)
    slope_hidden = jnp.dot(slope_out, down_matrix, preferred_element_type=jnp.float32) * H ** (-0.5)
    slope_pre = (slope_hidden * silu_slope(pre)).astype(jnp.bfloat16)
    return lax.dot_general(tokens_path, slope_pre, (((0,), (0,)), ((), ())), preferred_element_type=jnp.float32) * D ** (-0.5)

def grad_down(tokens_path, targets_path, up_matrix, down_matrix):
    pre, hidden_act, slope_out = forward(tokens_path, targets_path, up_matrix, down_matrix)
    return lax.dot_general(slope_out, hidden_act, (((0,), (0,)), ((), ())), preferred_element_type=jnp.float32) * H ** (-0.5)

def reference(tokens, targets, w_up, w_down, up_momentum, down_momentum, member_up, member_down, path_rate):
    token_grid = tokens.reshape(N_ROW, N_COL, ROWS, D)
    target_grid = targets.reshape(N_ROW, N_COL, ROWS, D)
    flags_up = member_up.astype(jnp.float32)
    flags_down = member_down.astype(jnp.float32)

    def phase_up(total, row_id):
        down_matrix = w_down[row_id]

        def one_path(tokens_path, targets_path, up_matrix, rate, flag):
            grad = grad_up(tokens_path, targets_path, up_matrix, down_matrix)
            quant, scales = packed(grad, rate)
            return flag * scales[:, None] * quant.astype(jnp.float32)
        terms = jax.vmap(one_path)(token_grid[row_id], target_grid[row_id], w_up, path_rate[row_id], flags_up[row_id])
        return (total + terms, None)
    start_up = jnp.zeros((N_COL, D, H), jnp.float32)
    total_up, unused = lax.scan(phase_up, start_up, jnp.arange(N_ROW, dtype=jnp.int32))
    average_up = total_up / lax.optimization_barrier(jnp.sum(flags_up, axis=0))[:, None, None]
    new_up_momentum = 0.9 * up_momentum + average_up
    new_up = (w_up.astype(jnp.float32) - 0.7 * (average_up + 0.9 * new_up_momentum)).astype(jnp.bfloat16)

    def phase_down(total, col_id):
        up_matrix = new_up[col_id]

        def one_path(tokens_path, targets_path, down_matrix, rate, flag):
            grad = grad_down(tokens_path, targets_path, up_matrix, down_matrix)
            quant, scales = packed(grad, rate)
            return flag * scales[:, None] * quant.astype(jnp.float32)
        terms = jax.vmap(one_path)(token_grid[:, col_id], target_grid[:, col_id], w_down, path_rate[:, col_id], flags_down[:, col_id])
        return (total + terms, None)
    start_down = jnp.zeros((N_ROW, D, H), jnp.float32)
    total_down, unused_down = lax.scan(phase_down, start_down, jnp.arange(N_COL, dtype=jnp.int32))
    average_down = total_down / lax.optimization_barrier(jnp.sum(flags_down, axis=1))[:, None, None]
    new_down_momentum = 0.9 * down_momentum + average_down
    new_down = (w_down.astype(jnp.float32) - 0.7 * (average_down + 0.9 * new_down_momentum)).astype(jnp.bfloat16)
    return (new_up, new_up_momentum, new_down, new_down_momentum)
```

```python
import jax
import jax.numpy as jnp
from jax import lax
from jax.sharding import PartitionSpec as P


def silu_slope(pre):
    sig = jax.nn.sigmoid(pre)
    return sig * (1.0 + pre * (1.0 - sig))


class Ring:
    def __init__(self, axis, size, stride):
        self.axis, self.size, self.stride = axis, size, stride
        self.paired = size & (size - 1) == 0
        self.place = lax.axis_index(axis) // stride

    def target(self, place, step):
        return place ^ step if self.paired else (place + step) % self.size

    def source(self, step):
        if self.paired:
            return self.place ^ step
        return lax.rem(self.place - step + self.size, self.size)

    def send(self, value, step):
        pairs = []
        for place in range(self.size):
            for core in range(self.stride):
                there = self.target(place, step)
                pairs.append((place * self.stride + core, there * self.stride + core))
        return lax.ppermute(value, self.axis, pairs)


def columns(array, index, width):
    return lax.dynamic_slice_in_dim(array, index * width, width, 1)


def path_sum(grads, factors):
    spread = jnp.sqrt(jnp.mean(grads * grads, axis=-1, keepdims=True) + 1e-05)
    unit = grads / (jnp.abs(grads) + spread)
    largest = jnp.max(jnp.abs(unit), axis=-1, keepdims=True) + 1e-06
    quant = (unit / largest).astype(jnp.bfloat16).astype(jnp.float32)
    return jnp.sum(factors[:, None, None] * largest * quant, axis=0)


def mm(a, b, dims):
    return lax.dot_general(a, b, (dims, ((), ())), preferred_element_type=jnp.float32)


def per_device(
    tokens, targets, w_up, w_down, up_momentum, down_momentum, member_up, member_down, path_rate
):
    width = tokens.shape[1]
    hidden = w_up.shape[2]
    inv_width = width ** (-0.5)
    inv_hidden = hidden ** (-0.5)
    row_count = lax.axis_size("row")
    col_count = lax.axis_size("col")
    row = Ring("row", row_count, 1)
    col = Ring("col", col_count // 2, 2)
    core = lax.rem(lax.axis_index("col"), 2)
    swap = [(i, i ^ 1) for i in range(col_count)]
    row_steps = range(1, row.size)
    col_steps = range(1, col.size)
    up_part = width // row.size
    down_part = width // col.size

    def sibling(value):
        return lax.ppermute(value, "col", swap)

    def pair(mine, other):
        first = jnp.where(core == 0, mine, other)
        second = jnp.where(core == 0, other, mine)
        return jnp.concatenate([first, second], axis=0)

    down_mine = w_down[0]
    down_sent = [down_mine] + [col.send(down_mine, s) for s in col_steps]
    inputs = [columns(tokens, row.source(0), up_part)]
    for s in row_steps:
        inputs.append(row.send(columns(tokens, row.target(row.place, s), up_part), s))
    down_pairs = [pair(block, sibling(block)) for block in down_sent]

    def forward(module, wire):
        total = mm(inputs[0], module, ((1,), (0,)))
        for s in row_steps:
            part = mm(inputs[s], module, ((1,), (0,))).astype(wire)
            back = s if row.paired else row.size - s
            total = total + row.send(part, back).astype(jnp.float32)
        return total * inv_width

    pre = forward(w_up[0], jnp.float32)
    hidden_act = jax.nn.silu(pre).astype(jnp.bfloat16)
    gaps = tokens.astype(jnp.float32) - targets.astype(jnp.float32)
    slope_hidden = 0.0
    for s, block in enumerate(down_pairs):
        here = col.source(s)
        gap = columns(tokens, here, down_part).astype(jnp.float32) - columns(
            targets, here, down_part
        ).astype(jnp.float32)
        slope_out = (gap + mm(hidden_act, block, ((1,), (1,))) * inv_hidden).astype(jnp.bfloat16)
        slope_hidden = slope_hidden + mm(slope_out, block, ((1,), (0,)))
    slope_pre = (slope_hidden * inv_hidden * silu_slope(pre)).astype(jnp.bfloat16)

    slopes = jnp.stack([slope_pre] + [row.send(slope_pre, s) for s in row_steps])
    gap_wire = gaps.astype(jnp.bfloat16)
    gap_wire, _ = lax.optimization_barrier((gap_wire, slope_pre))
    gap_parts = [columns(gap_wire, col.source(0), down_part)]
    for s in col_steps:
        gap_parts.append(col.send(columns(gap_wire, col.target(col.place, s), down_part), s))

    col_index = lax.axis_index("col")
    row_index = lax.axis_index("row")
    flags_up = lax.dynamic_index_in_dim(member_up, col_index, 1, False).astype(jnp.float32)
    factors = flags_up / jnp.sum(flags_up) * lax.dynamic_index_in_dim(path_rate, col_index, 1, False)
    factors_up = jnp.stack([factors[row.source(s)] for s in range(row.size)])
    grads_up = (
        jnp.einsum("srk,srh->skh", jnp.stack(inputs), slopes, preferred_element_type=jnp.float32)
        * inv_width
    )
    average_up = path_sum(grads_up, factors_up)
    momentum_first = 0.9 * up_momentum[0] + average_up
    fresh_up = (w_up[0].astype(jnp.float32) - 0.7 * (average_up + 0.9 * momentum_first)).astype(
        jnp.bfloat16
    )

    pre_again = forward(fresh_up, jnp.bfloat16)
    hidden_again = jax.nn.silu(pre_again).astype(jnp.bfloat16)
    hiddens = [hidden_again] + [col.send(hidden_again, s) for s in col_steps]
    flags_down = lax.dynamic_index_in_dim(member_down, row_index, 0, False).astype(jnp.float32)
    factors = flags_down / jnp.sum(flags_down) * lax.dynamic_index_in_dim(path_rate, row_index, 0, False)
    factors_down = jnp.stack([factors[col.source(s) * 2 + core] for s in range(col.size)])
    slopes_again = [
        (gap.astype(jnp.float32) + mm(act, down_pairs[0], ((1,), (1,))) * inv_hidden).astype(
            jnp.bfloat16
        )
        for gap, act in zip(gap_parts, hiddens)
    ]
    grads_down = (
        jnp.einsum(
            "srk,srh->skh",
            jnp.stack(slopes_again),
            jnp.stack(hiddens),
            preferred_element_type=jnp.float32,
        )
        * inv_hidden
    )
    sums = path_sum(grads_down, factors_down)
    rows = w_down.shape[1]
    mine = lax.dynamic_slice_in_dim(sums, core * rows, rows, 0)
    other = lax.dynamic_slice_in_dim(sums, (1 - core) * rows, rows, 0)
    average_down = mine + sibling(other)
    momentum_second = 0.9 * down_momentum[0] + average_down
    fresh_down = (
        w_down[0].astype(jnp.float32) - 0.7 * (average_down + 0.9 * momentum_second)
    ).astype(jnp.bfloat16)
    return (fresh_up[None], momentum_first[None], fresh_down[None], momentum_second[None])


def solution(mesh):
    placed = (
        P(("row", "col"), None),
        P(("row", "col"), None),
        P("col", "row", None),
        P("row", "col", None),
        P("col", "row", None),
        P("row", "col", None),
        P(),
        P(),
        P(),
    )
    return jax.shard_map(
        per_device,
        mesh=mesh,
        in_specs=placed,
        out_specs=(
            P("col", "row", None),
            P("col", "row", None),
            P("row", "col", None),
            P("row", "col", None),
        ),
        check_vma=False,
    )
```

```python
import functools

import jax
import jax.numpy as jnp
from jax import lax
from jax.experimental import pallas as pl
from jax.experimental.pallas import tpu as pltpu
from jax.sharding import PartitionSpec as P


BF16 = jnp.bfloat16
F32 = jnp.float32


def silu_slope(pre):
    sig = jax.nn.sigmoid(pre)
    return sig * (1.0 + pre * (1.0 - sig))


class Ring:
    def __init__(self, axis, size, stride):
        self.axis, self.size, self.stride = axis, size, stride
        self.paired = size & (size - 1) == 0
        self.place = lax.axis_index(axis) // stride

    def target(self, place, step):
        return place ^ step if self.paired else (place + step) % self.size

    def source(self, step):
        if self.paired:
            return lax.axis_index(self.axis) // self.stride ^ step
        return lax.rem(lax.axis_index(self.axis) // self.stride - step + self.size, self.size)

    def permute(self, value, places):
        pairs = []
        for place, there in places:
            for core in range(self.stride):
                pairs.append((place * self.stride + core, there * self.stride + core))
        return lax.ppermute(value, self.axis, pairs)

    def send(self, value, step):
        return self.permute(value, [(p, self.target(p, step)) for p in range(self.size)])

    def gather(self, value):
        if self.size != 4:
            return [value] + [self.send(value, s) for s in range(1, self.size)]
        two = self.send(value, 2)
        one = self.send(value, 1)
        inner = self.permute(value, [(1, 2), (2, 1)])
        outer = self.permute(two, [(2, 3), (1, 0)])
        end = (self.place == 0) | (self.place == 3)
        return [value, one, two, (end, outer, inner)]


def columns(array, index, width):
    return lax.dynamic_slice_in_dim(array, index * width, width, 1)


def mm(a, b, dims):
    return lax.dot_general(a, b, (dims, ((), ())), preferred_element_type=F32)


def kernel_call(body, outs, args, smem=(), alias=None, name=None, flops=10**8):
    vmem = pl.BlockSpec(memory_space=pltpu.VMEM)
    specs = [pl.BlockSpec(memory_space=pltpu.SMEM) if i in smem else vmem for i in range(len(args))]
    return pl.pallas_call(
        body,
        out_shape=[jax.ShapeDtypeStruct(*o) for o in outs],
        in_specs=specs,
        out_specs=[vmem] * len(outs),
        input_output_aliases=alias or {},
        compiler_params=pltpu.CompilerParams(vmem_limit_bytes=40 * 2**20),
        cost_estimate=pl.CostEstimate(flops=flops, transcendentals=0, bytes_accessed=2**20),
        name=name,
    )(*args)


def packed_sum(grad, axis, weight, count):
    size = grad.shape[axis]
    spread = jnp.sqrt(jnp.sum(grad * grad, axis=axis, keepdims=True) * (1.0 / size) + 1e-05)
    size_of = jnp.abs(grad)
    peak = jnp.max(size_of, axis=axis, keepdims=True)
    largest = peak / (peak + spread) + 1e-06
    quant = (grad / (size_of + spread) * (1.0 / largest)).astype(BF16).astype(F32)
    return largest * weight / count * quant


def down_piece(first, last, scale, swapped, *refs):
    refs = list(refs)
    gap, act, mine, other = refs[:4]
    rest = refs[4:]
    acc = None if first else rest.pop(0)
    pre = rest.pop(0) if last else None
    out, pair = rest
    rows = mine.shape[0]
    core = lax.rem(lax.axis_index("col"), 2)
    pair[pl.ds(pl.multiple_of(core * rows, 16), rows), :] = mine[...]
    pair[pl.ds(pl.multiple_of((1 - core) * rows, 16), rows), :] = other[...]
    block = pair[...]
    dy = (gap[...] + mm(act[...], block, ((0,), (1,))) * scale).astype(BF16)
    total = mm(dy, block, ((1,), (0,)))
    if not first:
        total = total + acc[...]
    if last:
        out[...] = (total.T * scale * silu_slope(pre[...])).astype(BF16)
    else:
        out[...] = total


def up_path(first, last, source, scale, *refs):
    refs = list(refs)
    member, rate, tokens, slope = refs[:4]
    rest = refs[4:]
    acc = None if first else rest.pop(0)
    path = source()
    place = lax.axis_index("col")
    count = member[0, place]
    for i in range(1, member.shape[0]):
        count = count + member[i, place]
    weight = member[path, place].astype(F32) * rate[path, place]
    grad = mm(slope[...], tokens[...], ((1,), (0,))) * scale
    total = packed_sum(grad, 0, weight, count.astype(F32))
    if not first:
        total = total + acc[...]
    if last:
        momentum, module, fresh, out = rest
        moved = 0.9 * momentum[...] + total
        fresh[...] = (module[...].astype(F32) - 0.7 * (total + 0.9 * moved)).astype(BF16)
        out[...] = total
    else:
        rest[0][...] = total


def down_path(first, last, source, scale, *refs):
    refs = list(refs)
    member, rate, gap, act, mine, other = refs[:6]
    rest = refs[6:]
    acc = None if first else rest.pop(0)
    pair = rest.pop()
    rows = mine.shape[0]
    core = lax.rem(lax.axis_index("col"), 2)
    pair[pl.ds(0, rows), :] = mine[...]
    pair[pl.ds(rows, rows), :] = other[...]
    path = source() * 2 + core
    place = lax.axis_index("row")
    count = member[place, 0]
    for i in range(1, member.shape[1]):
        count = count + member[place, i]
    weight = member[place, path].astype(F32) * rate[place, path]
    hid = act[...].astype(F32).T.astype(BF16)
    dy = (gap[...].astype(F32) + mm(hid, pair[...], ((1,), (1,))) * scale).astype(BF16)
    grad = mm(dy, hid, ((0,), (0,))) * scale
    total = packed_sum(grad, 1, weight, count.astype(F32))
    if not first:
        total = total + acc[...]
    if last:
        rest[0][...] = total[:rows]
        rest[1][...] = total[rows:]
    else:
        rest[0][...] = total


def per_device(
    tokens, targets, w_up, w_down, up_momentum, down_momentum, member_up, member_down, path_rate
):
    tokens_count, width = tokens.shape
    hidden = w_up.shape[2]
    inv_width = width ** (-0.5)
    inv_hidden = hidden ** (-0.5)
    col_count = lax.axis_size("col")
    row = Ring("row", lax.axis_size("row"), 1)
    col = Ring("col", col_count // 2, 2)
    core = lax.rem(lax.axis_index("col"), 2)
    swap = [(i, i ^ 1) for i in range(col_count)]
    row_steps = range(1, row.size)
    col_steps = range(1, col.size)
    up_part = width // row.size
    down_part = width // col.size
    rows = w_down.shape[1]

    def sibling(value):
        return lax.ppermute(value, "col", swap)

    blocks = []
    for block in col.gather(w_down[0]):
        if isinstance(block, tuple):
            block = jnp.where(*block)
        blocks.append((block, sibling(block)))
    inputs = [columns(tokens, row.source(0), up_part)]
    for s in row_steps:
        inputs.append(row.send(columns(tokens, row.target(row.place, s), up_part), s))

    def forward(module, wire):
        total = mm(module, inputs[0], ((1,), (1,)))
        for s in row_steps:
            part = mm(module, inputs[s], ((1,), (1,))).astype(wire)
            back = s if row.paired else row.size - s
            total = total + row.send(part, back).astype(F32)
        return total * inv_width

    module_up = w_up[0].T
    pre = forward(module_up, F32)
    act = jax.nn.silu(pre).astype(BF16)
    gaps = tokens.astype(F32) - targets.astype(F32)
    total = None
    for s in range(col.size):
        first, last = s == 0, s == col.size - 1
        mine, other = blocks[s]
        args = [columns(gaps, col.source(s), down_part), act, mine, other]
        if not first:
            args.append(total)
        if last:
            args.append(pre)
        total = pl.pallas_call(
            functools.partial(down_piece, first, last, inv_hidden, None),
            out_shape=jax.ShapeDtypeStruct(
                (hidden, tokens_count) if last else (tokens_count, hidden), BF16 if last else F32
            ),
            in_specs=[pl.BlockSpec(memory_space=pltpu.VMEM)] * len(args),
            out_specs=pl.BlockSpec(memory_space=pltpu.VMEM),
            scratch_shapes=[pltpu.VMEM((2 * rows, hidden), BF16)],
            compiler_params=pltpu.CompilerParams(vmem_limit_bytes=32 * 2**20),
            cost_estimate=pl.CostEstimate(
                flops=4 * tokens_count * hidden * down_part, transcendentals=0, bytes_accessed=2**21
            ),
            name=f"down_piece_{s}",
        )(*args)
    slope_pre = total

    slopes = [slope_pre] + [row.send(slope_pre, s) for s in row_steps]
    gap_wire, _ = lax.optimization_barrier((gaps.astype(BF16), slope_pre))
    gap_parts = [columns(gap_wire, col.source(0), down_part)]
    for s in col_steps:
        gap_parts.append(col.send(columns(gap_wire, col.target(col.place, s), down_part), s))

    average = None
    for s in range(row.size):
        first, last = s == 0, s == row.size - 1
        args = [member_up, path_rate, inputs[s], slopes[s]]
        alias = {}
        if not first:
            alias = {len(args): 1 if last else 0}
            args.append(average)
        outs = [((hidden, up_part), F32)]
        if last:
            args += [up_momentum[0].T, module_up]
            outs = [((hidden, up_part), BF16)] + outs
        result = kernel_call(
            functools.partial(up_path, first, last, functools.partial(row.source, s), inv_width),
            outs, args, (0, 1), alias, f"up_path_{s}",
        )
        average = result[-1]
    fresh = result[0]

    act = jax.nn.silu(forward(fresh, BF16)).astype(BF16)
    acts = [act] + [col.send(act, s) for s in col_steps]
    first_block = jnp.where(core == 0, blocks[0][0], blocks[0][1])
    second_block = jnp.where(core == 0, blocks[0][1], blocks[0][0])
    sums = None
    for s in range(col.size):
        first, last = s == 0, s == col.size - 1
        args = [member_down, path_rate, gap_parts[s], acts[s], first_block, second_block]
        if not first:
            args.append(sums)
        outs = [((rows, hidden), F32)] * 2 if last else [((2 * rows, hidden), F32)]
        sums = pl.pallas_call(
            functools.partial(down_path, first, last, functools.partial(col.source, s), inv_hidden),
            out_shape=[jax.ShapeDtypeStruct(*o) for o in outs],
            in_specs=[pl.BlockSpec(memory_space=pltpu.SMEM)] * 2
            + [pl.BlockSpec(memory_space=pltpu.VMEM)] * (len(args) - 2),
            out_specs=[pl.BlockSpec(memory_space=pltpu.VMEM)] * len(outs),
            scratch_shapes=[pltpu.VMEM((2 * rows, hidden), BF16)],
            input_output_aliases={} if first or last else {6: 0},
            compiler_params=pltpu.CompilerParams(vmem_limit_bytes=40 * 2**20),
            cost_estimate=pl.CostEstimate(flops=10**8, transcendentals=0, bytes_accessed=2**21),
            name=f"down_path_{s}",
        )(*args)
        if not last:
            sums = sums[0]
    mine = jnp.where(core == 0, sums[0], sums[1])
    other = jnp.where(core == 0, sums[1], sums[0])
    average_down = mine + sibling(other)
    momentum_second = 0.9 * down_momentum[0] + average_down
    fresh_down = (
        w_down[0].astype(F32) - 0.7 * (average_down + 0.9 * momentum_second)
    ).astype(BF16)
    momentum_first = 0.9 * up_momentum[0] + average.T
    return (fresh.T[None], momentum_first[None], fresh_down[None], momentum_second[None])


def solution(mesh):
    placed = (
        P(("row", "col"), None),
        P(("row", "col"), None),
        P("col", "row", None),
        P("row", "col", None),
        P("col", "row", None),
        P("row", "col", None),
        P(),
        P(),
        P(),
    )
    return jax.shard_map(
        per_device,
        mesh=mesh,
        in_specs=placed,
        out_specs=(
            P("col", "row", None),
            P("col", "row", None),
            P("row", "col", None),
            P("row", "col", None),
        ),
        check_vma=False,
    )
```

```python
import functools

import jax
import jax.numpy as jnp
from jax import lax
from jax.experimental import pallas as pl
from jax.experimental.pallas import tpu as pltpu
from jax.sharding import PartitionSpec as P


BF16 = jnp.bfloat16
F32 = jnp.float32


def silu_slope(pre):
    sig = jax.nn.sigmoid(pre)
    return sig * (1.0 + pre * (1.0 - sig))


class Ring:
    def __init__(self, axis, size, stride):
        self.axis, self.size, self.stride = axis, size, stride
        self.paired = size & (size - 1) == 0

    def target(self, place, step):
        return place ^ step if self.paired else (place + step) % self.size

    def aim(self, step):
        return self.target(lax.axis_index(self.axis) // self.stride, step)

    def source(self, step):
        if self.paired:
            return lax.axis_index(self.axis) // self.stride ^ step
        return lax.rem(lax.axis_index(self.axis) // self.stride - step + self.size, self.size)

    def back(self, step):
        return step if self.paired else self.size - step

    def permute(self, value, places):
        pairs = []
        for place, there in places:
            for core in range(self.stride):
                pairs.append((place * self.stride + core, there * self.stride + core))
        return lax.ppermute(value, self.axis, pairs)

    def send(self, value, step):
        return self.permute(value, [(p, self.target(p, step)) for p in range(self.size)])


def parity_pair(position, other):
    return 2 * position + (lax.axis_index("col") // 2 + other & 1)


def columns(array, index, width):
    return lax.dynamic_slice_in_dim(array, index * width, width, 1)


def mm(a, b, dims):
    return lax.dot_general(a, b, (dims, ((), ())), preferred_element_type=F32)


def kernel_call(body, outs, args, smem=(), alias=None, scratch=()):
    vmem = pl.BlockSpec(memory_space=pltpu.VMEM)
    specs = [pl.BlockSpec(memory_space=pltpu.SMEM) if i in smem else vmem for i in range(len(args))]
    return pl.pallas_call(
        body,
        out_shape=[jax.ShapeDtypeStruct(*o) for o in outs],
        in_specs=specs,
        out_specs=[vmem] * len(outs),
        scratch_shapes=scratch,
        input_output_aliases=alias or {},
        compiler_params=pltpu.CompilerParams(vmem_limit_bytes=12 * 2**20),
        cost_estimate=pl.CostEstimate(flops=10**8, transcendentals=0, bytes_accessed=2**20),
    )(*args)


def packed_sum(dots, scale, axis, weight, count):
    size = dots.shape[axis]
    square = jnp.sum(dots * dots, axis=axis, keepdims=True) * (1.0 / size)
    spread = jnp.sqrt(square + 1e-05 / scale**2)
    size_of = jnp.abs(dots)
    peak = jnp.max(size_of, axis=axis, keepdims=True)
    largest = peak / (peak + spread) + 1e-06
    inverse = 1.0 / largest
    quant = (dots * pl.reciprocal(size_of + spread) * inverse).astype(BF16).astype(F32)
    return largest * weight / count * quant


def cut_tokens(places, tokens, *refs):
    outs, sems = refs[:-1], refs[-1]
    copies = []
    for i, (place, out) in enumerate(zip(places, outs)):
        width = out.shape[1]
        block = tokens.at[:, pl.ds(pl.multiple_of(place() * width, 128), width)]
        copies.append(pltpu.make_async_copy(block, out, sems.at[i]))
        copies[-1].start()
    for copy in copies:
        copy.wait()


def split(own_pairs, next_pairs, later_pairs, tokens, targets, *outs):
    def cut(ref, place, width):
        return ref[:, pl.ds(pl.multiple_of(place() * width, 128), width)]

    here, following = outs[:2]
    width = here.shape[1] // len(own_pairs)

    def gap(place):
        return cut(tokens, place, width).astype(F32) - cut(targets, place, width).astype(F32)

    for out, places in ((here, own_pairs), (following, next_pairs)):
        for j, place in enumerate(places):
            out[:, j * width : (j + 1) * width] = gap(place).astype(out.dtype)
    for place, out in zip(later_pairs, outs[2:]):
        out[...] = gap(place).astype(out.dtype)


def part_product(module, tokens, out):
    out[...] = mm(module[...], tokens[...], ((1,), (1,))).astype(out.dtype)


def activate(scale, *refs):
    count = len(refs) - (2 if refs[-1].dtype == F32 else 1)
    total = refs[0][...]
    for ref in refs[1:count]:
        total = total + ref[...].astype(F32)
    total = total * scale
    refs[count][...] = jax.nn.silu(total).astype(BF16)
    if count + 2 == len(refs):
        refs[-1][...] = total


def stack_gap(step, own, following, out):
    width = own.shape[1]
    out[0] = own[...]
    out[1] = read_gap(following, (step, width))


def read_gap(ref, where):
    if where is None:
        return ref[...]
    if isinstance(where, int):
        return ref[where]
    step, width = where
    place = lax.axis_index("col") // 4 ^ step
    return ref[:, pl.ds(pl.multiple_of(place * width, 128), width)]


def assemble(half, *refs):
    out = refs[-1]
    rows = refs[0].shape[0]
    place = lax.axis_index("col") // 2
    core = lax.rem(lax.axis_index("col"), 2)
    for s in range(half):
        base = ((place >> 1) ^ s) * (2 * rows)
        mine = pl.multiple_of(base + core * rows, 16)
        other = pl.multiple_of(base + (1 - core) * rows, 16)
        out[pl.ds(mine, rows), :] = refs[2 * s][...]
        out[pl.ds(other, rows), :] = refs[2 * s + 1][...]


def half_slope(scale, gap, act, module, out):
    whole = module[...]
    dy = (gap[...].astype(F32) + mm(act[...], whole, ((0,), (1,))) * scale).astype(BF16)
    out[...] = mm(dy, whole, ((1,), (0,))).astype(out.dtype)


def join_slope(scale, here, there, pre, out):
    total = here[...] + there[...].astype(F32)
    out[...] = (total.T * scale * silu_slope(pre[...])).astype(BF16)


def up_path(first, last, source, scale, *refs):
    refs = list(refs)
    member, rate, tokens, slope = refs[:4]
    rest = refs[4:]
    acc = None if first else rest.pop(0)
    path = source()
    place = lax.axis_index("col")
    count = member[0, place]
    for i in range(1, member.shape[0]):
        count = count + member[i, place]
    weight = member[path, place].astype(F32) * rate[path, place]
    dots = mm(slope[...], tokens[...], ((1,), (0,)))
    total = packed_sum(dots, scale, 0, weight, count.astype(F32))
    if not first:
        total = total + acc[...]
    if last:
        count = (len(rest) - 3) // 2
        momentum, module = rest[:2]
        inputs = rest[2 : 2 + count]
        parts = rest[2 + count : -1]
        rest[-1][...] = total
        moved = 0.9 * momentum[...] + total
        fresh = (module[...].astype(F32) - 0.7 * (total + 0.9 * moved)).astype(BF16)
        for token_part, part in zip(list(inputs) + [tokens], parts):
            part[...] = mm(fresh, token_part[...], ((1,), (1,))).astype(part.dtype)
    else:
        rest[0][...] = total


def outer_update(average, momentum, module, fresh, moved):
    total = average[...]
    moment = 0.9 * momentum[...] + total
    moved[...] = moment
    fresh[...] = (module[...].astype(F32) - 0.7 * (total + 0.9 * moment)).astype(BF16)


def pair_update(mine, other, momentum, module, fresh, moved):
    total = mine[...] + other[...]
    moment = 0.9 * momentum[...] + total
    moved[...] = moment
    fresh[...] = (module[...].astype(F32) - 0.7 * (total + 0.9 * moment)).astype(BF16)


def down_factor(member, rate, path):
    place = lax.axis_index("row")
    count = member[place, 0]
    for i in range(1, member.shape[1]):
        count = count + member[place, i]
    return member[place, path].astype(F32) * rate[place, path], count.astype(F32)


def own_rows(module, half):
    count = module.shape[0] // half
    place = lax.axis_index("col") // 4
    return module[pl.ds(pl.multiple_of(place * count, 16), count), :]


def down_path(first, half, where, source, scale, *refs):
    member, rate, gap, act, module = refs[:5]
    weight, count = down_factor(member, rate, source() * 2 + lax.rem(lax.axis_index("col"), 2))
    hid = act[...].astype(F32).T.astype(BF16)
    dy = (read_gap(gap, where).astype(F32) + mm(hid, own_rows(module, half), ((1,), (1,))) * scale).astype(BF16)
    total = packed_sum(mm(dy, hid, ((0,), (0,))), scale, 1, weight, count)
    if not first:
        total = total + refs[5][...]
    refs[-1][...] = total


def down_last(half, where, source, scale, member, rate, gap, act, module, acc, other, slopes):
    core = lax.rem(lax.axis_index("col"), 2)
    weight, count = down_factor(member, rate, source() * 2 + core)
    hid = act[...].astype(F32).T.astype(BF16)
    dy = read_gap(gap, where).astype(F32) + mm(hid, own_rows(module, half), ((1,), (1,))) * scale
    slopes[...] = dy.T.astype(BF16)
    rows = other.shape[0]
    part = pl.ds(pl.multiple_of((1 - core) * rows, 16), rows)
    total = packed_sum(mm(slopes[part, :], hid, ((1,), (0,))), scale, 1, weight, count)
    other[...] = total + acc[part, :]


def down_mine(source, scale, member, rate, slopes, act, acc, mine):
    core = lax.rem(lax.axis_index("col"), 2)
    weight, count = down_factor(member, rate, source() * 2 + core)
    hid = act[...].astype(F32).T.astype(BF16)
    rows = mine.shape[0]
    part = pl.ds(pl.multiple_of(core * rows, 16), rows)
    total = packed_sum(mm(slopes[part, :], hid, ((1,), (0,))), scale, 1, weight, count)
    mine[...] = total + acc[part, :]


def per_device(
    tokens, targets, w_up, w_down, up_momentum, down_momentum, member_up, member_down, path_rate
):
    tokens_count, width = tokens.shape
    hidden = w_up.shape[2]
    inv_width = width ** (-0.5)
    inv_hidden = hidden ** (-0.5)
    col_count = lax.axis_size("col")
    row = Ring("row", lax.axis_size("row"), 1)
    col = Ring("col", col_count // 2, 2)
    core = lax.rem(lax.axis_index("col"), 2)
    swap = [(i, i ^ 1) for i in range(col_count)]
    row_steps = range(1, row.size)
    col_steps = range(1, col.size)
    up_part = width // row.size
    down_part = width // col.size
    rows = w_down.shape[1]

    def sibling(value):
        return lax.ppermute(value, "col", swap)

    half = col.size // 2

    row_places = [functools.partial(row.aim, s) for s in range(row.size)]
    own_pairs = [functools.partial(parity_pair, j, 0) for j in range(half)]
    next_pairs = [functools.partial(parity_pair, j, 1) for j in range(half)]
    later_pairs = [functools.partial(col.aim, 2 * s) for s in range(half)]
    shapes = [((tokens_count, up_part), BF16)] * row.size
    shapes += [((tokens_count, half * down_part), t) for t in (F32, BF16)]
    shapes += [((tokens_count, down_part), BF16)] * half
    if up_part % 128 or down_part % 128:
        def gap(place):
            return columns(tokens, place(), down_part).astype(F32) - columns(
                targets, place(), down_part
            ).astype(F32)

        cuts = [columns(tokens, place(), up_part) for place in row_places]
        cuts.append(jnp.concatenate([gap(p) for p in own_pairs], axis=1))
        cuts.append(jnp.concatenate([gap(p) for p in next_pairs], axis=1).astype(BF16))
        cuts += [gap(p).astype(BF16) for p in later_pairs]
    else:
        cuts = pl.pallas_call(
            functools.partial(cut_tokens, row_places),
            out_shape=[jax.ShapeDtypeStruct(*o) for o in shapes[: row.size]],
            in_specs=[pl.BlockSpec(memory_space=pl.ANY)],
            out_specs=[pl.BlockSpec(memory_space=pltpu.VMEM)] * row.size,
            scratch_shapes=[pltpu.SemaphoreType.DMA((row.size,))],
            compiler_params=pltpu.CompilerParams(vmem_limit_bytes=2 * 2**20),
            name="cut_tokens",
        )(tokens)
        cuts += kernel_call(
            functools.partial(split, own_pairs, next_pairs, later_pairs),
            shapes[row.size :], [tokens, targets],
        )
    gap_here, gap_next = cuts[row.size : row.size + 2]
    gap_later = cuts[row.size + 2 :]
    inputs = [cuts[0]]
    for s in row_steps:
        inputs.append(row.send(cuts[s], s))

    module_up = w_up[0].T
    flat = (hidden, tokens_count)
    parts = []
    for s in range(row.size):
        (part,) = kernel_call(part_product, [(flat, BF16 if s else F32)], [module_up, inputs[s]])
        if s:
            part = row.send(part, row.back(s))
        parts.append(part)
    act, pre = kernel_call(
        functools.partial(activate, inv_width), [(flat, BF16), (flat, F32)], parts
    )

    blocks = []
    for s in range(half):
        if s:
            block = col.send(w_down[0], 2 * s)
        else:
            block = w_down[0]
        blocks += [block, sibling(block)]
    (module_half,) = kernel_call(
        functools.partial(assemble, half),
        [((half * 2 * rows, hidden), BF16)], blocks,
    )
    gap_next = col.send(gap_next, 1)
    act_next = col.send(act, 1)
    shape = (tokens_count, hidden)
    (there,) = kernel_call(
        functools.partial(half_slope, inv_hidden),
        [(shape, BF16)], [gap_next, act_next, module_half],
    )
    (here,) = kernel_call(
        functools.partial(half_slope, inv_hidden),
        [(shape, F32)], [gap_here, act, module_half],
    )
    there = col.send(there, 1)
    (slope_pre,) = kernel_call(
        functools.partial(join_slope, inv_hidden),
        [((hidden, tokens_count), BF16)], [here, there, pre],
    )

    slopes = [slope_pre] + [row.send(slope_pre, s) for s in row_steps]
    aligned = down_part % 128 == 0
    gap_parts = [(gap_later[0], None), (gap_next, (0, down_part))]
    for s in range(1, half):
        wide = (2, tokens_count, down_part)
        if aligned:
            (both,) = kernel_call(
                functools.partial(stack_gap, s), [(wide, BF16)], [gap_later[s], gap_next],
            )
        else:
            place = lax.axis_index("col") // 4 ^ s
            both = jnp.stack([gap_later[s], columns(gap_next, place, down_part)])
        both = col.send(both, 2 * s)
        gap_parts += [(both, 0), (both, 1)]
    if not aligned:
        gap_parts[1] = (columns(gap_next, lax.axis_index("col") // 4, down_part), None)

    average = None
    for s in range(row.size):
        first, last = s == 0, s == row.size - 1
        args = [member_up, path_rate, inputs[s], slopes[s]]
        alias = {}
        outs = [((hidden, up_part), F32)]
        if not first:
            alias = {len(args): row.size if last else 0}
            args.append(average)
        if last:
            args += [up_momentum[0].T, module_up] + inputs[:-1]
            shape = (hidden, tokens_count)
            outs = [(shape, F32)] + [(shape, BF16)] * (row.size - 1) + outs
        result = kernel_call(
            functools.partial(up_path, first, last, functools.partial(row.source, s), inv_width),
            outs, args, (0, 1), alias,
        )
        average = result[-1]
    fresh, moved = kernel_call(
        outer_update,
        [((hidden, up_part), BF16), ((hidden, up_part), F32)],
        [average, up_momentum[0].T, module_up],
    )

    parts = [result[0]]
    for s in row_steps:
        parts.append(row.send(result[s], row.back(s)))
    (act,) = kernel_call(functools.partial(activate, inv_width), [(flat, BF16)], parts)
    acts = [act] + [col.send(act, s) for s in col_steps]
    sums = None
    for s in range(col.size - 1):
        args = [member_down, path_rate, gap_parts[s][0], acts[s], module_half] + ([sums] if s else [])
        (sums,) = kernel_call(
            functools.partial(down_path, s == 0, half, gap_parts[s][1], functools.partial(col.source, s), inv_hidden),
            [((2 * rows, hidden), F32)], args, (0, 1), {5: 0} if s else {},
        )
    source = functools.partial(col.source, col.size - 1)
    other, slopes_last = kernel_call(
        functools.partial(down_last, half, gap_parts[-1][1], source, inv_hidden),
        [((rows, hidden), F32), ((2 * rows, tokens_count), BF16)],
        [member_down, path_rate, gap_parts[-1][0], acts[-1], module_half, sums],
        (0, 1),
    )
    (mine,) = kernel_call(
        functools.partial(down_mine, source, inv_hidden),
        [((rows, hidden), F32)],
        [member_down, path_rate, slopes_last, acts[-1], sums],
        (0, 1),
    )
    fresh_down, moved_down = kernel_call(
        pair_update,
        [((rows, hidden), BF16), ((rows, hidden), F32)],
        [mine, sibling(other), down_momentum[0], w_down[0]],
    )
    return (fresh.T[None], moved.T[None], fresh_down[None], moved_down[None])


def solution(mesh):
    placed = (
        P(("row", "col"), None),
        P(("row", "col"), None),
        P("col", "row", None),
        P("row", "col", None),
        P("col", "row", None),
        P("row", "col", None),
        P(),
        P(),
        P(),
    )
    return jax.shard_map(
        per_device,
        mesh=mesh,
        in_specs=placed,
        out_specs=(
            P("col", "row", None),
            P("col", "row", None),
            P("row", "col", None),
            P("row", "col", None),
        ),
        check_vma=False,
    )
```

```python
import functools

import jax
import jax.numpy as jnp
from jax import lax
from jax.experimental import pallas as pl
from jax.experimental.pallas import tpu as pltpu
from jax.sharding import PartitionSpec as P


BF16 = jnp.bfloat16
F32 = jnp.float32


def silu_slope(pre):
    sig = jax.nn.sigmoid(pre)
    return sig * (1.0 + pre * (1.0 - sig))


class Ring:
    def __init__(self, axis, size, stride):
        self.axis, self.size, self.stride = axis, size, stride
        self.paired = size & (size - 1) == 0

    def target(self, place, step):
        return place ^ step if self.paired else (place + step) % self.size

    def aim(self, step):
        return self.target(lax.axis_index(self.axis) // self.stride, step)

    def source(self, step):
        if self.paired:
            return lax.axis_index(self.axis) // self.stride ^ step
        return lax.rem(lax.axis_index(self.axis) // self.stride - step + self.size, self.size)

    def back(self, step):
        return step if self.paired else self.size - step

    def permute(self, value, places):
        pairs = []
        for place, there in places:
            for core in range(self.stride):
                pairs.append((place * self.stride + core, there * self.stride + core))
        return lax.ppermute(value, self.axis, pairs)

    def send(self, value, step):
        return self.permute(value, [(p, self.target(p, step)) for p in range(self.size)])


def parity_pair(position, other):
    return 2 * position + (lax.axis_index("col") // 2 + other & 1)


def columns(array, index, width):
    return lax.dynamic_slice_in_dim(array, index * width, width, 1)


def mm(a, b, dims):
    return lax.dot_general(a, b, (dims, ((), ())), preferred_element_type=F32)


def kernel_call(body, outs, args, smem=(), alias=None, scratch=()):
    vmem = pl.BlockSpec(memory_space=pltpu.VMEM)
    specs = [pl.BlockSpec(memory_space=pltpu.SMEM) if i in smem else vmem for i in range(len(args))]
    return pl.pallas_call(
        body,
        out_shape=[jax.ShapeDtypeStruct(*o) for o in outs],
        in_specs=specs,
        out_specs=[vmem] * len(outs),
        scratch_shapes=scratch,
        input_output_aliases=alias or {},
        compiler_params=pltpu.CompilerParams(vmem_limit_bytes=12 * 2**20),
        cost_estimate=pl.CostEstimate(flops=10**8, transcendentals=0, bytes_accessed=2**20),
    )(*args)


def packed_sum(dots, scale, axis, weight, count):
    size = dots.shape[axis]
    square = jnp.sum(dots * dots, axis=axis, keepdims=True) * (1.0 / size)
    spread = jnp.sqrt(square + 1e-05 / scale**2)
    size_of = jnp.abs(dots)
    peak = jnp.max(size_of, axis=axis, keepdims=True)
    largest = peak / (peak + spread) + 1e-06
    inverse = 1.0 / largest
    quant = (dots * pl.reciprocal(size_of + spread) * inverse).astype(BF16).astype(F32)
    return largest * weight / count * quant


def cut(ref, place, width):
    return ref[:, pl.ds(pl.multiple_of(place() * width, 128), width)]


def cut_tokens(places, tokens, *outs):
    for place, out in zip(places, outs):
        out[...] = cut(tokens, place, out.shape[1])
    outs[-1][...] = tokens[...]


def split(own_pairs, next_pairs, later_pairs, tokens, targets, *outs):
    here, following = outs[:2]
    width = here.shape[1] // len(own_pairs)

    def gap(place):
        return cut(tokens, place, width).astype(F32) - cut(targets, place, width).astype(F32)

    for out, places in ((here, own_pairs), (following, next_pairs)):
        for j, place in enumerate(places):
            out[:, j * width : (j + 1) * width] = gap(place).astype(out.dtype)
    for place, out in zip(later_pairs, outs[2:]):
        out[...] = gap(place).astype(out.dtype)


def part_product(module, tokens, out):
    out[...] = mm(module[...], tokens[...], ((1,), (1,))).astype(out.dtype)


def activate(scale, *refs):
    count = len(refs) - (2 if refs[-1].dtype == F32 else 1)
    total = refs[0][...]
    for ref in refs[1:count]:
        total = total + ref[...].astype(F32)
    total = total * scale
    refs[count][...] = jax.nn.silu(total).astype(BF16)
    if count + 2 == len(refs):
        refs[-1][...] = total


def stack_gap(step, own, following, out):
    width = own.shape[1]
    out[0] = own[...]
    out[1] = read_gap(following, (step, width))


def read_gap(ref, where):
    if where is None:
        return ref[...]
    if isinstance(where, int):
        return ref[where]
    step, width = where
    place = lax.axis_index("col") // 4 ^ step
    return ref[:, pl.ds(pl.multiple_of(place * width, 128), width)]


def assemble(half, *refs):
    out = refs[-1]
    rows = refs[0].shape[0]
    place = lax.axis_index("col") // 2
    core = lax.rem(lax.axis_index("col"), 2)
    for s in range(half):
        base = ((place >> 1) ^ s) * (2 * rows)
        mine = pl.multiple_of(base + core * rows, 16)
        other = pl.multiple_of(base + (1 - core) * rows, 16)
        out[pl.ds(mine, rows), :] = refs[2 * s][...]
        out[pl.ds(other, rows), :] = refs[2 * s + 1][...]


def half_slope(scale, gap, act, module, out):
    whole = module[...]
    dy = (gap[...].astype(F32) + mm(act[...], whole, ((0,), (1,))) * scale).astype(BF16)
    out[...] = mm(dy, whole, ((1,), (0,))).astype(out.dtype)


def join_slope(scale, here, there, pre, out):
    total = here[...] + there[...].astype(F32)
    out[...] = (total.T * scale * silu_slope(pre[...])).astype(BF16)


def up_path(first, last, source, scale, *refs):
    refs = list(refs)
    member, rate, tokens, slope = refs[:4]
    rest = refs[4:]
    acc = None if first else rest.pop(0)
    path = source()
    place = lax.axis_index("col")
    count = member[0, place]
    for i in range(1, member.shape[0]):
        count = count + member[i, place]
    weight = member[path, place].astype(F32) * rate[path, place]
    dots = mm(slope[...], tokens[...], ((1,), (0,)))
    total = packed_sum(dots, scale, 0, weight, count.astype(F32))
    if not first:
        total = total + acc[...]
    if last:
        count = (len(rest) - 3) // 2
        momentum, module = rest[:2]
        inputs = rest[2 : 2 + count]
        parts = rest[2 + count : -1]
        rest[-1][...] = total
        moved = 0.9 * momentum[...] + total
        fresh = (module[...].astype(F32) - 0.7 * (total + 0.9 * moved)).astype(BF16)
        together = jnp.concatenate([ref[...] for ref in inputs] + [tokens[...]], axis=0)
        products = mm(fresh, together, ((1,), (1,)))
        wide = tokens.shape[0]
        for i, part in enumerate(parts):
            part[...] = products[:, i * wide : (i + 1) * wide].astype(part.dtype)
    else:
        rest[0][...] = total


def outer_update(average, momentum, module, fresh, moved):
    total = average[...]
    moment = 0.9 * momentum[...] + total
    moved[...] = moment
    fresh[...] = (module[...].astype(F32) - 0.7 * (total + 0.9 * moment)).astype(BF16)


def pair_update(mine, other, momentum, module, fresh, moved):
    total = mine[...] + other[...].astype(F32)
    moment = 0.9 * momentum[...] + total
    moved[...] = moment
    fresh[...] = (module[...].astype(F32) - 0.7 * (total + 0.9 * moment)).astype(BF16)


def down_factor(member, rate, path):
    place = lax.axis_index("row")
    count = member[place, 0]
    for i in range(1, member.shape[1]):
        count = count + member[place, i]
    return member[place, path].astype(F32) * rate[place, path], count.astype(F32)


def own_rows(module, half):
    count = module.shape[0] // half
    place = lax.axis_index("col") // 4
    return module[pl.ds(pl.multiple_of(place * count, 16), count), :]


def down_path(first, half, where, source, scale, *refs):
    member, rate, gap, act, module = refs[:5]
    weight, count = down_factor(member, rate, source() * 2 + lax.rem(lax.axis_index("col"), 2))
    hid = act[...].astype(F32).T.astype(BF16)
    dy = (read_gap(gap, where).astype(F32) + mm(hid, own_rows(module, half), ((1,), (1,))) * scale).astype(BF16)
    total = packed_sum(mm(dy, hid, ((0,), (0,))), scale, 1, weight, count)
    if not first:
        total = total + refs[5][...]
    refs[-1][...] = total


def down_last(half, where, source, scale, member, rate, gap, act, module, acc, other, slopes):
    core = lax.rem(lax.axis_index("col"), 2)
    weight, count = down_factor(member, rate, source() * 2 + core)
    hid = act[...].astype(F32).T.astype(BF16)
    dy = read_gap(gap, where).astype(F32) + mm(hid, own_rows(module, half), ((1,), (1,))) * scale
    slopes[...] = dy.T.astype(BF16)
    rows = other.shape[0]
    part = pl.ds(pl.multiple_of((1 - core) * rows, 16), rows)
    total = packed_sum(mm(slopes[part, :], hid, ((1,), (0,))), scale, 1, weight, count)
    other[...] = (total + acc[part, :]).astype(other.dtype)


def down_mine(source, scale, member, rate, slopes, act, acc, mine):
    core = lax.rem(lax.axis_index("col"), 2)
    weight, count = down_factor(member, rate, source() * 2 + core)
    hid = act[...].astype(F32).T.astype(BF16)
    rows = mine.shape[0]
    part = pl.ds(pl.multiple_of(core * rows, 16), rows)
    total = packed_sum(mm(slopes[part, :], hid, ((1,), (0,))), scale, 1, weight, count)
    mine[...] = total + acc[part, :]


def per_device(
    tokens, targets, w_up, w_down, up_momentum, down_momentum, member_up, member_down, path_rate
):
    tokens_count, width = tokens.shape
    hidden = w_up.shape[2]
    inv_width = width ** (-0.5)
    inv_hidden = hidden ** (-0.5)
    col_count = lax.axis_size("col")
    row = Ring("row", lax.axis_size("row"), 1)
    col = Ring("col", col_count // 2, 2)
    core = lax.rem(lax.axis_index("col"), 2)
    swap = [(i, i ^ 1) for i in range(col_count)]
    row_steps = range(1, row.size)
    col_steps = range(1, col.size)
    up_part = width // row.size
    down_part = width // col.size
    rows = w_down.shape[1]

    def sibling(value):
        return lax.ppermute(value, "col", swap)

    half = col.size // 2

    row_places = [functools.partial(row.aim, s) for s in range(row.size)]
    own_pairs = [functools.partial(parity_pair, j, 0) for j in range(half)]
    next_pairs = [functools.partial(parity_pair, j, 1) for j in range(half)]
    later_pairs = [functools.partial(col.aim, 2 * s) for s in range(half)]
    shapes = [((tokens_count, up_part), BF16)] * row.size
    shapes += [((tokens_count, half * down_part), t) for t in (F32, BF16)]
    shapes += [((tokens_count, down_part), BF16)] * half
    if up_part % 128 or down_part % 128:
        def gap(place):
            return columns(tokens, place(), down_part).astype(F32) - columns(
                targets, place(), down_part
            ).astype(F32)

        cuts = [columns(tokens, place(), up_part) for place in row_places]
        cuts.append(jnp.concatenate([gap(p) for p in own_pairs], axis=1))
        cuts.append(jnp.concatenate([gap(p) for p in next_pairs], axis=1).astype(BF16))
        cuts += [gap(p).astype(BF16) for p in later_pairs]
    else:
        *cuts, staged = kernel_call(
            functools.partial(cut_tokens, row_places),
            shapes[: row.size] + [(tokens.shape, BF16)], [tokens],
        )
        cuts += kernel_call(
            functools.partial(split, own_pairs, next_pairs, later_pairs),
            shapes[row.size :], [staged, targets],
        )
    gap_here, gap_next = cuts[row.size : row.size + 2]
    gap_later = cuts[row.size + 2 :]
    inputs = [cuts[0]]
    for s in row_steps:
        inputs.append(row.send(cuts[s], s))

    module_up = w_up[0].T
    flat = (hidden, tokens_count)
    parts = []
    for s in range(row.size):
        (part,) = kernel_call(part_product, [(flat, BF16 if s else F32)], [module_up, inputs[s]])
        if s:
            part = row.send(part, row.back(s))
        parts.append(part)
    act, pre = kernel_call(
        functools.partial(activate, inv_width), [(flat, BF16), (flat, F32)], parts
    )

    blocks = []
    for s in range(half):
        if s:
            block = col.send(w_down[0], 2 * s)
        else:
            block = w_down[0]
        blocks += [block, sibling(block)]
    (module_half,) = kernel_call(
        functools.partial(assemble, half),
        [((half * 2 * rows, hidden), BF16)], blocks,
    )
    gap_next = col.send(gap_next, 1)
    act_next = col.send(act, 1)
    shape = (tokens_count, hidden)
    (there,) = kernel_call(
        functools.partial(half_slope, inv_hidden),
        [(shape, BF16)], [gap_next, act_next, module_half],
    )
    (here,) = kernel_call(
        functools.partial(half_slope, inv_hidden),
        [(shape, F32)], [gap_here, act, module_half],
    )
    there = col.send(there, 1)
    (slope_pre,) = kernel_call(
        functools.partial(join_slope, inv_hidden),
        [((hidden, tokens_count), BF16)], [here, there, pre],
    )

    slopes = [slope_pre] + [row.send(slope_pre, s) for s in row_steps]
    aligned = down_part % 128 == 0
    gap_parts = [(gap_later[0], None), (gap_next, (0, down_part))]
    for s in range(1, half):
        wide = (2, tokens_count, down_part)
        if aligned:
            (both,) = kernel_call(
                functools.partial(stack_gap, s), [(wide, BF16)], [gap_later[s], gap_next],
            )
        else:
            place = lax.axis_index("col") // 4 ^ s
            both = jnp.stack([gap_later[s], columns(gap_next, place, down_part)])
        both = col.send(both, 2 * s)
        gap_parts += [(both, 0), (both, 1)]
    if not aligned:
        gap_parts[1] = (columns(gap_next, lax.axis_index("col") // 4, down_part), None)

    average = None
    for s in range(row.size):
        first, last = s == 0, s == row.size - 1
        args = [member_up, path_rate, inputs[s], slopes[s]]
        alias = {}
        outs = [((hidden, up_part), F32)]
        if not first:
            alias = {len(args): row.size if last else 0}
            args.append(average)
        if last:
            args += [up_momentum[0].T, module_up] + inputs[:-1]
            shape = (hidden, tokens_count)
            outs = [(shape, F32)] + [(shape, BF16)] * (row.size - 1) + outs
        result = kernel_call(
            functools.partial(up_path, first, last, functools.partial(row.source, s), inv_width),
            outs, args, (0, 1), alias,
        )
        average = result[-1]
    fresh, moved = kernel_call(
        outer_update,
        [((hidden, up_part), BF16), ((hidden, up_part), F32)],
        [average, up_momentum[0].T, module_up],
    )

    parts = [result[0]]
    for s in row_steps:
        parts.append(row.send(result[s], row.back(s)))
    (act,) = kernel_call(functools.partial(activate, inv_width), [(flat, BF16)], parts)
    acts = [act] + [col.send(act, s) for s in col_steps]
    sums = None
    for s in range(col.size - 1):
        args = [member_down, path_rate, gap_parts[s][0], acts[s], module_half] + ([sums] if s else [])
        (sums,) = kernel_call(
            functools.partial(down_path, s == 0, half, gap_parts[s][1], functools.partial(col.source, s), inv_hidden),
            [((2 * rows, hidden), F32)], args, (0, 1), {5: 0} if s else {},
        )
    source = functools.partial(col.source, col.size - 1)
    other, slopes_last = kernel_call(
        functools.partial(down_last, half, gap_parts[-1][1], source, inv_hidden),
        [((rows, hidden), BF16), ((2 * rows, tokens_count), BF16)],
        [member_down, path_rate, gap_parts[-1][0], acts[-1], module_half, sums],
        (0, 1),
    )
    (mine,) = kernel_call(
        functools.partial(down_mine, source, inv_hidden),
        [((rows, hidden), F32)],
        [member_down, path_rate, slopes_last, acts[-1], sums],
        (0, 1),
    )
    fresh_down, moved_down = kernel_call(
        pair_update,
        [((rows, hidden), BF16), ((rows, hidden), F32)],
        [mine, sibling(other), down_momentum[0], w_down[0]],
    )
    return (fresh.T[None], moved.T[None], fresh_down[None], moved_down[None])


def solution(mesh):
    placed = (
        P(("row", "col"), None),
        P(("row", "col"), None),
        P("col", "row", None),
        P("row", "col", None),
        P("col", "row", None),
        P("row", "col", None),
        P(),
        P(),
        P(),
    )
    return jax.shard_map(
        per_device,
        mesh=mesh,
        in_specs=placed,
        out_specs=(
            P("col", "row", None),
            P("col", "row", None),
            P("row", "col", None),
            P("row", "col", None),
        ),
        check_vma=False,
    )
```
